256 devices in a mesh: section: 2 (over x_hi), feat: 16 (over y, x_lo, core), width: 8 (over z).
Axes of the slice: x: 4 (x_hi: 2, x_lo: 2; x = x_hi * 2 + x_lo), y: 4, z: 8, core: 2. Of those that a mesh axis runs over, the one named last changes fastest.
Arguments:
- mlp_inputs: bfloat16 [4, 1024, 2304], P('section', 'width'), may hold values from -6 to 6
- encoder: bfloat16 [4, 2304, 16384], P('section', 'width', 'feat'), may hold values from -0.125 to 0.125
- enc_bias: float32 [4, 16384], P('section', 'feat'), may hold values from -3 to 3
- decoder: bfloat16 [10, 16384, 2304], P('section', 'feat', 'width'), may hold values from -0.046875 to 0.046875
- dec_bias: float32 [4, 2304], P(None, 'width'), may hold values from -3 to 3
- targets: bfloat16 [4, 1024, 2304], P(None, None, 'width'), may hold values from -6 to 6
- live_rows: int32 [1024], replicated, may hold values 0 or 1
Outputs:
- errors: bfloat16 [4, 1024, 2304], P(None, None, 'width')
- gradients: bfloat16 [10, 16384, 2304], P('section', 'feat', 'width')
The draws below stay inside these ranges and needn't reach their ends.
All inputs are finite; a program needn't handle non-finite values.
Results may differ from the reference program's by a relative error of at most 0.0042.
Values may be sent and summed in bfloat16 or wider, within the bound.
No kernel may reach another device: no remote copies, remote signals or barrier semaphores. Data moves between devices by JAX's collectives and lax.ppermute only.
A program may use at most 128 MiB of HBM per device.

```python
import jax
import jax.numpy as jnp

D = 2304
F = 16384
TOKENS = 1024
LAYERS = 4
PAIRS = 10


def with_ends(values, key, smallest, largest):
    longest = values.shape.index(max(values.shape))
    spots = []
    for shift in (0, 1):
        where = [jax.random.randint(jax.random.fold_in(key, axis), (), 0, length) for axis, length in enumerate(values.shape)]
        where[longest] = (where[longest] + shift) % values.shape[longest]
        spots.append(tuple(where))
    return values.at[spots[0]].set(smallest).at[spots[1]].set(largest)


def block_scale(stream_key, shape, shards, smallest, high):
    def one(position, shards_of):
        heights = jax.random.uniform(jax.random.fold_in(jax.random.fold_in(stream_key, 6), position), (shards_of,), jnp.float32, smallest / len(shards), high / len(shards))
        return jnp.repeat(jnp.exp(heights), shape[position] // shards_of).reshape((-1,) + (1,) * (len(shape) - position - 1))

    loudness = one(*shards[0])
    for cut in shards[1:]:
        loudness = loudness * one(*cut)
    return loudness


def normal_values(own_key, extent, scale, most, shards=(), kind=jnp.bfloat16):
    values = jax.random.normal(own_key, extent, jnp.float32) * scale
    if len(shards) > 0:
        values = block_scale(own_key, extent, shards, -0.22, 0.18) * values
    return jnp.clip(values, min=-most, max=most).astype(kind)


def setup_inputs(seed: int = 0) -> dict:
    seeds = jax.random.split(jax.random.key(seed), 8)
    return {
        "mlp_inputs": normal_values(seeds[0], (LAYERS, TOKENS, D), 1.0, 6.0, ((0, 2), (1, 8))),
        "encoder": normal_values(seeds[1], (LAYERS, D, F), D ** -0.5, 0.125, ((0, 2), (1, 8), (2, 16))),
        "enc_bias": normal_values(seeds[2], (LAYERS, F), 0.5, 3.0, ((0, 2), (1, 16)), jnp.float32),
        "decoder": normal_values(seeds[3], (PAIRS, F, D), F ** -0.5, 0.046875, ((0, 2), (1, 16), (2, 8))),
        "dec_bias": normal_values(seeds[4], (LAYERS, D), 0.5, 3.0, ((1, 8),), jnp.float32),
        "targets": normal_values(seeds[5], (LAYERS, TOKENS, D), 1.0, 6.0, ((2, 8),)),
        "live_rows": with_ends((jax.random.randint(seeds[6], (TOKENS,), 0, 8) < 7).astype(jnp.int32), jax.random.fold_in(seeds[6], 1), 0, 1),
    }


def pair_list(layer_count):
    return [(source, target) for source in range(layer_count) for target in range(source, layer_count)]


def reference(mlp_inputs, encoder, enc_bias, decoder, dec_bias, targets, live_rows):
    features = []
    for layer_id in range(LAYERS):
        pre_act = jnp.dot(mlp_inputs[layer_id], encoder[layer_id], preferred_element_type=jnp.float32) + enc_bias[layer_id]
        features.append(jnp.maximum(pre_act, 0.0).astype(jnp.bfloat16))
    rebuilt = [jnp.zeros((TOKENS, D), jnp.float32) for target in range(LAYERS)]
    for pair_id, (source, target) in enumerate(pair_list(LAYERS)):
        rebuilt[target] = rebuilt[target] + jnp.dot(features[source], decoder[pair_id], preferred_element_type=jnp.float32)
    keep_rows = live_rows.astype(jnp.float32)[:, None]
    errors = jnp.stack([(rebuilt[target] + dec_bias[target] - targets[target].astype(jnp.float32)) * keep_rows for target in range(LAYERS)]).astype(jnp.bfloat16)
    gradients = []
    for pair_id, (source, target) in enumerate(pair_list(LAYERS)):
        product = jnp.dot(features[source].T, errors[target], preferred_element_type=jnp.float32)
        gradients.append((product / TOKENS).astype(jnp.bfloat16))
    return errors, jnp.stack(gradients)
```

```python
import jax
import jax.numpy as jnp
from jax import lax
from jax.sharding import PartitionSpec as P

PLANE = ("section", "feat")
BF16 = jnp.bfloat16
F32 = jnp.float32


def place(x, y, core):
    return (x // 2) * 16 + (y * 2 + x % 2) * 2 + core


def plane_pairs(move):
    pairs = []
    for x in range(4):
        for y in range(4):
            for core in range(2):
                x2, y2, core2 = move(x, y, core)
                pairs.append((place(x, y, core), place(x2 % 4, y2 % 4, core2)))
    return pairs


def along_x(value, steps):
    return lax.ppermute(value, PLANE, plane_pairs(lambda x, y, c: (x + steps, y, c)))


def along_y(value, steps):
    return lax.ppermute(value, PLANE, plane_pairs(lambda x, y, c: (x, y + steps, c)))


def other_core(value):
    return lax.ppermute(value, PLANE, plane_pairs(lambda x, y, c: (x, y, 1 - c)))


def coords():
    section = lax.axis_index("section")
    feat = lax.axis_index("feat")
    return section * 2 + (feat // 2) % 2, feat // 4, feat % 2


def gather_ring4(block, me, axis, shift):
    rows = block.shape[axis]
    arrived = [(step, shift(block, step)) for step in (1, 3, 2)]
    shape = list(block.shape)
    shape[axis] *= 4
    whole = lax.dynamic_update_slice_in_dim(jnp.zeros(shape, block.dtype), block, me * rows, axis)
    for step, value in arrived:
        whole = lax.dynamic_update_slice_in_dim(whole, value, ((me - step) % 4) * rows, axis)
    return whole


def along_z(value, steps):
    count = lax.axis_size("width")
    return lax.ppermute(value, "width", [(z, (z + steps) % count) for z in range(count)])


def other_x(value):
    return lax.ppermute(value, PLANE, plane_pairs(lambda x, y, c: (x ^ 1, y, c)))


DIRECT = (1, 7, 2, 6, 3, 5, 4)


def pick(value, which):
    return lax.dynamic_index_in_dim(value, which, 0, keepdims=False)


def gather_inputs(mlp_inputs):
    x, y, core = coords()
    z = lax.axis_index("width")
    layers_here, tok_local, model_width = mlp_inputs.shape
    rows = tok_local // 8
    slab = lax.dynamic_slice(
        mlp_inputs, (x % 2, (y * 2 + core) * rows, 0), (1, rows, model_width)
    )
    with jax.named_scope("inputs_z"):
        arrived = [(step, along_z(slab, step)) for step in DIRECT]
    column = jnp.zeros((8, rows, model_width), BF16)
    column = lax.dynamic_update_slice(column, slab, (z, 0, 0))
    for step, value in arrived:
        column = lax.dynamic_update_slice(column, value, ((z - step) % 8, 0, 0))
    column = column[:, None]
    with jax.named_scope("inputs_y"):
        arrived = [(step, along_y(column, step)) for step in (1, 3, 2)]
    plane = jnp.zeros((8, 4, rows, model_width), BF16)
    plane = lax.dynamic_update_slice(plane, column, (0, y, 0, 0))
    for step, value in arrived:
        plane = lax.dynamic_update_slice(plane, value, (0, (y - step) % 4, 0, 0))
    plane = plane[:, :, None]
    with jax.named_scope("inputs_core"):
        swapped = other_core(plane)
    tokens = jnp.zeros((8, 4, 2, rows, model_width), BF16)
    tokens = lax.dynamic_update_slice(tokens, plane, (0, 0, core, 0, 0))
    tokens = lax.dynamic_update_slice(tokens, swapped, (0, 0, 1 - core, 0, 0))
    return tokens.reshape(8 * tok_local, model_width)


def spread_encoder(near, far):
    z = lax.axis_index("width")
    depth, columns = near.shape
    lanes = columns // 8
    both = jnp.stack([near, far])

    def block(to):
        return lax.dynamic_slice(both, (0, 0, to * lanes), (2, depth, lanes))

    with jax.named_scope("encoder_z"):
        arrived = [(step, along_z(block((z + step) % 8), step)) for step in DIRECT]
    whole = jnp.zeros((2, 8, depth, lanes), BF16)
    whole = lax.dynamic_update_slice(whole, block(z)[:, None], (0, z, 0, 0))
    for step, value in arrived:
        whole = lax.dynamic_update_slice(whole, value[:, None], (0, (z - step) % 8, 0, 0))
    return whole.reshape(2, 8 * depth, lanes)


def encode(mlp_inputs, encoder, enc_bias):
    x, y, core = coords()
    z = lax.axis_index("width")
    own = x % 2
    with jax.named_scope("encoder_x"):
        far_cols = other_x(pick(encoder, 1 - own))
    with jax.named_scope("bias_x"):
        far_bias = other_x(pick(enc_bias, 1 - own))
    tokens = gather_inputs(mlp_inputs)
    spread = spread_encoder(pick(encoder, own), far_cols)
    lanes = spread.shape[2]

    def activate(cols, bias):
        shift = lax.dynamic_slice_in_dim(bias, z * lanes, lanes, 0)
        pre_act = jnp.dot(tokens, cols, preferred_element_type=F32)
        return jnp.maximum(pre_act + shift[None, :], 0.0).astype(BF16)

    kept = activate(spread[0], pick(enc_bias, own))
    with jax.named_scope("features_x"):
        swapped = other_x(activate(spread[1], far_bias))
    return kept, swapped


def ring_blocks(block, last):
    blocks = {0: block}
    up = down = block
    for step in range(1, 4):
        with jax.named_scope("ring"):
            up, down = along_z(up, 1), along_z(down, -1)
        blocks[step], blocks[8 - step] = up, down
    with jax.named_scope("ring"):
        blocks[4] = along_z(up, 1) if last == 1 else along_z(down, -1)
    return blocks


def assemble(blocks):
    z = lax.axis_index("width")
    tokens_all, lanes = blocks[0].shape
    whole = jnp.zeros((tokens_all, 8 * lanes), BF16)
    for behind in (0, 1, 7, 2, 6, 3, 5, 4):
        whole = lax.dynamic_update_slice(whole, blocks[behind], (0, ((z - behind) % 8) * lanes))
    return whole


def send_ahead(first, second, odd, groups):
    z = lax.axis_index("width")
    tokens_all, lanes = first[0].shape
    whole = jnp.zeros((tokens_all, 8 * lanes), BF16)
    for group in groups:
        piece = jnp.stack([jnp.where(odd, first[b], second[b]) for b in group])
        with jax.named_scope("ahead"):
            piece = lax.ppermute(piece, "section", [(0, 1)])
        for spot, behind in enumerate(group):
            whole = lax.dynamic_update_slice(
                whole, piece[spot], (0, ((z - behind) % 8) * lanes)
            )
    return whole


def plan_decoders(decoder, first_section, odd):
    with jax.named_scope("decoder_back"):
        back = lax.ppermute(decoder[:2], "section", [(1, 0)])
    zero = jnp.zeros(decoder.shape[1:], BF16)
    near = (
        jnp.where(first_section, decoder[0], zero),
        jnp.where(first_section, decoder[1], zero),
        decoder[2],
        decoder[3],
    )
    far = (
        zero,
        jnp.where(first_section, decoder[4], zero),
        back[0],
        jnp.where(first_section, back[1], decoder[4]),
    )
    own = jnp.stack([jnp.where(odd, f, n) for n, f in zip(near, far)])
    other = jnp.stack([jnp.where(odd, n, f) for n, f in zip(near, far)])
    return own, other


def decode(own, other, own_dec, other_dec, first, rows):
    a = lax.dynamic_slice_in_dim(own, first, rows, 0)
    b = lax.dynamic_slice_in_dim(other, first, rows, 0)
    return [
        jnp.dot(a, own_dec[m], preferred_element_type=F32)
        + jnp.dot(b, other_dec[m], preferred_element_type=F32)
        for m in range(own_dec.shape[0])
    ]


def reduce_errors(own, other, own_dec, other_dec, dec_bias, targets, live_rows):
    x, y, core = coords()
    half = own.shape[0] // 2
    rows = half // 4
    sent = jnp.stack(decode(own, other, own_dec, other_dec, (1 - core) * half, half))
    with jax.named_scope("sum_core"):
        arrived = other_core(sent)
    kept = jnp.stack(decode(own, other, own_dec, other_dec, core * half, half))

    def quarter(to):
        return lax.dynamic_slice_in_dim(kept, to * rows, rows, 1) + lax.dynamic_slice_in_dim(
            arrived, to * rows, rows, 1
        )

    with jax.named_scope("sum_y"):
        parts = [along_y(quarter((y + step) % 4).astype(BF16), step) for step in (1, 3, 2)]
    total = quarter(y)
    for part in parts:
        total = total + part.astype(F32)
    with jax.named_scope("sum_x"):
        parts = [along_x(pick(total, (x + step) % 4), step) for step in (1, 3, 2)]
    total = pick(total, x)
    for part in parts:
        total = total + part
    first = core * half + y * rows
    wanted = lax.dynamic_slice(targets, (x, first, 0), (1, rows, targets.shape[2]))[0].astype(F32)
    live = lax.dynamic_slice_in_dim(live_rows, first, rows, 0).astype(F32)
    errors = ((total + pick(dec_bias, x)[None, :] - wanted) * live[:, None]).astype(BF16)[None]
    with jax.named_scope("errors_x"):
        errors = gather_ring4(errors, x, 0, along_x)
    with jax.named_scope("errors_y"):
        errors = gather_ring4(errors, y, 1, along_y)
    with jax.named_scope("errors_core"):
        swapped = other_core(errors)
    low = jnp.where(core == 0, errors, swapped)
    high = jnp.where(core == 0, swapped, errors)
    return jnp.concatenate([low, high], axis=1)


def local(mlp_inputs, encoder, enc_bias, decoder, dec_bias, targets, live_rows):
    tokens_all = live_rows.shape[0]
    x, y, core = coords()
    first_section = x < 2
    odd = x % 2 == 1
    own_dec, other_dec = plan_decoders(decoder, first_section, odd)
    kept, swapped = encode(mlp_inputs, encoder, enc_bias)
    own_blocks = ring_blocks(kept, 1)
    other_blocks = ring_blocks(swapped, -1)
    earlier = send_ahead(own_blocks, other_blocks, odd, ((0, 1, 7), (2, 6), (3, 5, 4)))
    own, other = assemble(own_blocks), assemble(other_blocks)
    errors = reduce_errors(own, other, own_dec, other_dec, dec_bias, targets, live_rows)
    near, far = jnp.where(odd, other, own), jnp.where(odd, own, other)
    lead = jnp.where(first_section, near, earlier)

    def gradient(features, residual):
        product = lax.dot_general(
            features, residual, (((0,), (0,)), ((), ())), preferred_element_type=F32
        )
        return (product / tokens_all).astype(BF16)

    gradients = [
        gradient(lead, jnp.where(first_section, errors[0], errors[2])),
        gradient(lead, jnp.where(first_section, errors[1], errors[3])),
        gradient(near, errors[2]),
        gradient(near, errors[3]),
        gradient(far, jnp.where(first_section, errors[1], errors[3])),
    ]
    return (errors, jnp.stack(gradients))


def solution(mesh):
    placed = (
        P("section", "width", None),
        P("section", "width", "feat"),
        P("section", "feat"),
        P("section", "feat", "width"),
        P(None, "width"),
        P(None, None, "width"),
        P(),
    )
    return jax.shard_map(
        local,
        mesh=mesh,
        in_specs=placed,
        out_specs=(P(None, None, "width"), P("section", "feat", "width")),
        check_vma=False,
    )
```

```python
import jax
import jax.numpy as jnp
from jax import lax
from jax.experimental import pallas as pl
from jax.experimental.pallas import tpu as pltpu
from jax.sharding import PartitionSpec as P


PLANE = ("section", "feat")
BF16 = jnp.bfloat16
F32 = jnp.float32
U32 = jnp.uint32
DIRECT = (1, 7, 2, 6, 3, 5, 4)
EARLY = (0, 1, 7, 2, 6, 3, 5)


def place(x, y, core):
    return (x // 2) * 16 + (y * 2 + x % 2) * 2 + core


def plane_pairs(move):
    pairs = []
    for x in range(4):
        for y in range(4):
            for core in range(2):
                x2, y2, core2 = move(x, y, core)
                pairs.append((place(x, y, core), place(x2 % 4, y2 % 4, core2)))
    return pairs


def along_x(value, steps):
    return lax.ppermute(value, PLANE, plane_pairs(lambda x, y, c: (x + steps, y, c)))


def along_y(value, steps):
    return lax.ppermute(value, PLANE, plane_pairs(lambda x, y, c: (x, y + steps, c)))


def along_z(value, steps):
    return lax.ppermute(value, "width", [(z, (z + steps) % 8) for z in range(8)])


def other_core(value):
    return lax.ppermute(value, PLANE, plane_pairs(lambda x, y, c: (x, y, 1 - c)))


def other_x(value):
    return lax.ppermute(value, PLANE, plane_pairs(lambda x, y, c: (x ^ 1, y, c)))


def coords():
    section = lax.axis_index("section").astype(U32)
    feat = lax.axis_index("feat").astype(U32)
    z = lax.axis_index("width").astype(U32)
    return section * 2 + ((feat >> 1) & 1), feat >> 2, z, feat & 1


def cut(value, axis, start, size):
    starts = [U32(0)] * value.ndim
    starts[axis] = start
    sizes = list(value.shape)
    sizes[axis] = size
    return lax.dynamic_slice(value, starts, sizes)


def pick(value, which):
    return cut(value, 0, which, 1)[0]


def put(whole, value, axis, start):
    starts = [U32(0)] * whole.ndim
    starts[axis] = start
    return lax.dynamic_update_slice(whole, value, starts)


def gather_inputs(mlp_inputs, own):
    _, y, _, core = coords()
    _, tok_local, model_width = mlp_inputs.shape
    rows = tok_local // 8
    slab = lax.dynamic_slice(
        mlp_inputs, (own, (y * 2 + core) * rows, U32(0)), (1, rows, model_width)
    )
    column = lax.all_gather(slab[0], "width", axis=0, tiled=False)
    column = column[:, None]
    arrived = [(step, along_y(column, step)) for step in (1, 3, 2)]
    plane = put(jnp.zeros((8, 4, rows, model_width), BF16), column, 1, y)
    for step, value in arrived:
        plane = put(plane, value, 1, (y - step) & 3)
    plane = plane[:, :, None]
    swapped = other_core(plane)
    tokens = put(jnp.zeros((8, 4, 2, rows, model_width), BF16), plane, 2, core)
    tokens = put(tokens, swapped, 2, 1 - core)
    return tokens.reshape(8 * tok_local, model_width)


def spread_encoder(near, far):
    z = lax.axis_index("width").astype(U32)
    depth, columns = near.shape
    lanes = columns // 8

    def block(to):
        return jnp.concatenate([cut(near, 1, to * lanes, lanes), cut(far, 1, to * lanes, lanes)], 1)

    arrived = [(step, along_z(block((z + step) & 7), step)) for step in DIRECT]
    whole = put(jnp.zeros((8, depth, 2 * lanes), BF16), block(z)[None], 0, z)
    for step, value in arrived:
        whole = put(whole, value[None], 0, (z - step) & 7)
    return whole.reshape(8 * depth, 2 * lanes)


def encode(mlp_inputs, encoder, enc_bias):
    x, _, z, _ = coords()
    own = x & 1
    far_bias = other_x(pick(enc_bias, 1 - own))
    far_cols = other_x(pick(encoder, 1 - own))
    tokens = gather_inputs(mlp_inputs, own)
    spread = spread_encoder(pick(encoder, own), far_cols)
    lanes = spread.shape[1] // 2
    bias = [cut(value, 0, z * lanes, lanes) for value in (pick(enc_bias, own), far_bias)]
    pre_act = jnp.dot(tokens, spread, preferred_element_type=F32) + jnp.concatenate(bias)[None, :]
    active = lax.optimization_barrier(jnp.maximum(pre_act, 0.0).astype(BF16))
    kept = active[:, :lanes]
    swapped = other_x(active[:, lanes:])
    even = own == 0
    return jnp.stack([jnp.where(even, kept, swapped), jnp.where(even, swapped, kept)])


def ring_blocks(block):
    blocks = {0: block}
    up = down = block
    for step in range(1, 4):
        up, down = along_z(up, 1), along_z(down, 7)
        blocks[step], blocks[8 - step] = up, down
    up, down = along_z(up[:1], 1), along_z(down[1:], 7)
    blocks[4] = (up[0], down[0])
    return blocks


def assemble(blocks, layer):
    z = lax.axis_index("width").astype(U32)
    tokens_all, lanes = blocks[0][0].shape
    whole = jnp.zeros((tokens_all, 8 * lanes), BF16)
    for behind in (0, 1, 7, 2, 6, 3, 5, 4):
        whole = put(whole, blocks[behind][layer], 1, ((z - behind) & 7) * lanes)
    return whole


def send_ahead(blocks):
    early = jnp.concatenate([blocks[b][1] for b in EARLY])
    early = lax.ppermute(early, "section", [(0, 1)])
    late = lax.ppermute(blocks[4][1], "section", [(0, 1)])
    return early, late


def plan_decoders(decoder, first_section):
    back = lax.ppermute(decoder[:2], "section", [(1, 0)])
    slots, back = jnp.swapaxes(decoder, 1, 2), jnp.swapaxes(back, 1, 2)
    zero = jnp.zeros(slots.shape[1:], BF16)
    near = jnp.concatenate([jnp.where(first_section, slots[:2], zero), slots[2:4]])
    far = jnp.stack(
        [
            zero,
            jnp.where(first_section, slots[4], zero),
            back[0],
            jnp.where(first_section, back[1], slots[4]),
        ]
    )
    return near.reshape(-1, near.shape[2]), far.reshape(-1, far.shape[2])


def reduce_errors(features, decoders, dec_bias, targets, live_rows):
    x, y, _, core = coords()
    layers_all, width = dec_bias.shape
    half = live_rows.shape[0] // 2
    rows = half // 4

    def decode(first):
        rebuilt = sum(
            lax.dot_general(
                decoders[layer], cut(features[layer], 0, first, half), (((1,), (1,)), ((), ())),
                preferred_element_type=F32,
            )
            for layer in (0, 1)
        )
        return rebuilt.reshape(layers_all, width, half)

    arrived = other_core(decode((1 - core) * half))
    kept = decode(core * half)

    def quarter(to):
        return cut(kept, 2, to * rows, rows) + cut(arrived, 2, to * rows, rows)

    parts = [along_y(quarter((y + step) & 3).astype(BF16), step) for step in (1, 3, 2)]
    total = quarter(y)
    for part in parts:
        total = total + part.astype(F32)
    parts = [along_x(pick(total, (x + step) & 3), step) for step in (1, 3, 2)]
    total = pick(total, x)
    for part in parts:
        total = total + part
    first = core * half + y * rows
    wanted = lax.dynamic_slice(targets, (x, first, U32(0)), (1, rows, width))[0].T.astype(F32)
    live = cut(live_rows, 0, first, rows).astype(F32)
    errors = ((total + pick(dec_bias, x)[:, None] - wanted) * live[None, :]).astype(BF16)[None]

    def gather(block, me, axis, shift):
        arrived = [(step, shift(block, step)) for step in (1, 3, 2)]
        size = block.shape[axis]
        shape = list(block.shape)
        shape[axis] *= 4
        whole = put(jnp.zeros(shape, BF16), block, axis, me * size)
        for step, value in arrived:
            whole = put(whole, value, axis, ((me - step) & 3) * size)
        return whole

    errors = gather(errors, x, 0, along_x)
    errors = gather(errors, y, 2, along_y)
    swapped = other_core(errors)
    whole = put(jnp.zeros((layers_all, width, 2 * half), BF16), errors, 2, core * half)
    return put(whole, swapped, 2, (1 - core) * half)


def gradient_kernel(
    where_ref, errors_ref, near_ref, far_ref, early0_ref, early1_ref, late_ref, out_ref
):
    tile = pl.program_id(0)
    section = where_ref[16]
    width, tokens_all = errors_ref.shape[1:]
    scale = 1.0 / tokens_all
    halves = [
        jnp.where(where_ref[8 + 2 * tile + half] == 1, late_ref[...], early_ref[...])
        for half, early_ref in enumerate((early0_ref, early1_ref))
    ]
    near = near_ref[...]
    lead = jnp.where(section == 0, near, jnp.concatenate(halves, axis=1))

    def product(first, count, source):
        residual = errors_ref[pl.ds(first, count)].reshape(count * width, tokens_all)
        value = jnp.dot(residual, source, preferred_element_type=F32) * scale
        return value.astype(BF16).reshape(count, width, source.shape[1])

    out_ref[0:2] = product(2 * section, 2, lead)
    out_ref[2:4] = product(2, 2, near)
    out_ref[4:5] = product(1 + 2 * section, 1, far_ref[...])


def all_gradients(errors, near, far, early, late):
    _, width, tokens_all = errors.shape
    columns = near.shape[1]
    lanes = late.shape[1]
    z = lax.axis_index("width")
    section = lax.axis_index("section")
    spots = [EARLY.index(behind) if behind in EARLY else 0 for behind in range(8)]
    behind = (z - jnp.arange(8, dtype=jnp.int32)) & 7
    spot = sum(jnp.where(behind == b, spots[b], 0) for b in range(8))
    where = jnp.concatenate([spot, (behind == 4).astype(jnp.int32), section[None].astype(jnp.int32)])
    source = pl.BlockSpec((tokens_all, 2 * lanes), lambda i, where: (0, i))
    return pl.pallas_call(
        gradient_kernel,
        grid_spec=pltpu.PrefetchScalarGridSpec(
            num_scalar_prefetch=1,
            grid=(columns // (2 * lanes),),
            in_specs=[
                pl.BlockSpec(errors.shape, lambda i, where: (0, 0, 0)),
                source,
                source,
                pl.BlockSpec((tokens_all, lanes), lambda i, where: (where[2 * i], 0)),
                pl.BlockSpec((tokens_all, lanes), lambda i, where: (where[2 * i + 1], 0)),
                pl.BlockSpec((tokens_all, lanes), lambda i, where: (0, 0)),
            ],
            out_specs=pl.BlockSpec((5, width, 2 * lanes), lambda i, where: (0, 0, i)),
        ),
        out_shape=jax.ShapeDtypeStruct((5, width, columns), BF16),
        cost_estimate=pl.CostEstimate(
            flops=10 * width * tokens_all * columns, bytes_accessed=12000000, transcendentals=0
        ),
        name="gradients",
    )(where, errors, near, far, early, early, late)


def local(mlp_inputs, encoder, enc_bias, decoder, dec_bias, targets, live_rows):
    x, _, _, _ = coords()
    first_section = x < 2
    block = encode(mlp_inputs, encoder, enc_bias)
    decoders = plan_decoders(decoder, first_section)
    blocks = ring_blocks(block)
    early, late = send_ahead(blocks)
    near, far = assemble(blocks, 0), assemble(blocks, 1)
    errors = reduce_errors((near, far), decoders, dec_bias, targets, live_rows)
    gradients = all_gradients(errors, near, far, early, late)
    return jnp.swapaxes(errors, 1, 2), jnp.swapaxes(gradients, 1, 2)


def solution(mesh):
    placed = (
        P("section", "width", None),
        P("section", "width", "feat"),
        P("section", "feat"),
        P("section", "feat", "width"),
        P(None, "width"),
        P(None, None, "width"),
        P(),
    )
    return jax.shard_map(
        local,
        mesh=mesh,
        in_specs=placed,
        out_specs=(P(None, None, "width"), P("section", "feat", "width")),
        check_vma=False,
    )
```

```python
import jax
import jax.numpy as jnp
from jax import lax
from jax.experimental import pallas as pl
from jax.experimental.pallas import tpu as pltpu
from jax.sharding import PartitionSpec as P


PLANE = ("section", "feat")
BF16 = jnp.bfloat16
F32 = jnp.float32
U32 = jnp.uint32
DIRECT = (1, 7, 2, 6, 3, 5, 4)
EARLY = (0, 1, 7, 2, 6, 3, 5)


def place(x, y, core):
    return (x // 2) * 16 + (y * 2 + x % 2) * 2 + core


def plane_pairs(move):
    pairs = []
    for x in range(4):
        for y in range(4):
            for core in range(2):
                x2, y2, core2 = move(x, y, core)
                pairs.append((place(x, y, core), place(x2 % 4, y2 % 4, core2)))
    return pairs


def along_x(value, steps):
    return lax.ppermute(value, PLANE, plane_pairs(lambda x, y, c: (x + steps, y, c)))


def along_y(value, steps):
    return lax.ppermute(value, PLANE, plane_pairs(lambda x, y, c: (x, y + steps, c)))


def along_z(value, steps):
    return lax.ppermute(value, "width", [(z, (z + steps) % 8) for z in range(8)])


def other_core(value):
    return lax.ppermute(value, PLANE, plane_pairs(lambda x, y, c: (x, y, 1 - c)))


def other_x(value):
    return lax.ppermute(value, PLANE, plane_pairs(lambda x, y, c: (x ^ 1, y, c)))


def coords():
    section = lax.axis_index("section").astype(U32)
    feat = lax.axis_index("feat").astype(U32)
    z = lax.axis_index("width").astype(U32)
    return section * 2 + ((feat >> 1) & 1), feat >> 2, z, feat & 1


def cut(value, axis, start, size):
    starts = [U32(0)] * value.ndim
    starts[axis] = start
    sizes = list(value.shape)
    sizes[axis] = size
    return lax.dynamic_slice(value, starts, sizes)


def pick(value, which):
    return cut(value, 0, which, 1)[0]


def put(whole, value, axis, start):
    starts = [U32(0)] * whole.ndim
    starts[axis] = start
    return lax.dynamic_update_slice(whole, value, starts)


def gather_inputs(mlp_inputs, own):
    _, y, _, core = coords()
    _, tok_local, model_width = mlp_inputs.shape
    rows = tok_local // 8
    slab = lax.dynamic_slice(
        mlp_inputs, (own, (y * 2 + core) * rows, U32(0)), (1, rows, model_width)
    )
    column = lax.all_gather(slab[0], "width", axis=0, tiled=False)
    column = column[:, None]
    arrived = [(step, along_y(column, step)) for step in (1, 3, 2)]
    plane = put(jnp.zeros((8, 4, rows, model_width), BF16), column, 1, y)
    for step, value in arrived:
        plane = put(plane, value, 1, (y - step) & 3)
    plane = plane[:, :, None]
    swapped = other_core(plane)
    tokens = put(jnp.zeros((8, 4, 2, rows, model_width), BF16), plane, 2, core)
    tokens = put(tokens, swapped, 2, 1 - core)
    return tokens.reshape(8 * tok_local, model_width)


def spread_encoder(near, far):
    z = lax.axis_index("width").astype(U32)
    depth, columns = near.shape
    lanes = columns // 8

    def block(to):
        return jnp.concatenate([cut(near, 1, to * lanes, lanes), cut(far, 1, to * lanes, lanes)], 1)

    arrived = [(step, along_z(block((z + step) & 7), step)) for step in DIRECT]
    whole = put(jnp.zeros((8, depth, 2 * lanes), BF16), block(z)[None], 0, z)
    for step, value in arrived:
        whole = put(whole, value[None], 0, (z - step) & 7)
    return whole.reshape(8 * depth, 2 * lanes)


def encode(mlp_inputs, encoder, enc_bias):
    x, _, z, _ = coords()
    own = x & 1
    far_bias = other_x(pick(enc_bias, 1 - own))
    far_cols = other_x(pick(encoder, 1 - own))
    tokens = gather_inputs(mlp_inputs, own)
    spread = spread_encoder(pick(encoder, own), far_cols)
    lanes = spread.shape[1] // 2
    bias = [cut(value, 0, z * lanes, lanes) for value in (pick(enc_bias, own), far_bias)]
    pre_act = jnp.dot(tokens, spread, preferred_element_type=F32) + jnp.concatenate(bias)[None, :]
    active = lax.optimization_barrier(jnp.maximum(pre_act, 0.0).astype(BF16))
    kept = active[:, :lanes]
    swapped = other_x(active[:, lanes:])
    even = own == 0
    pair = jnp.stack([jnp.where(even, kept, swapped), jnp.where(even, swapped, kept)])
    return lax.optimization_barrier(pair)


def ring_blocks(block):
    blocks = {0: block}
    up = down = block
    for step in range(1, 4):
        up, down = along_z(up, 1), along_z(down, 7)
        blocks[step], blocks[8 - step] = up, down
    up, down = along_z(up[:1], 1), along_z(down[1:], 7)
    blocks[4] = (up[0], down[0])
    return blocks


def assemble(blocks):
    z = lax.axis_index("width").astype(U32)
    tokens_all, lanes = blocks[0][0].shape
    whole = jnp.zeros((tokens_all, 16 * lanes), BF16)
    for behind in (0, 1, 7, 2, 6, 3, 5, 4):
        for layer in (0, 1):
            whole = put(whole, blocks[behind][layer], 1, (((z - behind) & 7) + 8 * layer) * lanes)
    return whole


def send_ahead(blocks):
    early = jnp.concatenate([blocks[b][1] for b in EARLY])
    early = lax.ppermute(early, "section", [(0, 1)])
    late = lax.ppermute(blocks[4][1], "section", [(0, 1)])
    return early, late


def plan_decoders(decoder, first_section):
    back = lax.ppermute(decoder[:2], "section", [(1, 0)])
    slots, back = jnp.swapaxes(decoder, 1, 2), jnp.swapaxes(back, 1, 2)
    zero = jnp.zeros(slots.shape[1:], BF16)
    near = jnp.concatenate([jnp.where(first_section, slots[:2], zero), slots[2:4]])
    far = jnp.stack(
        [
            zero,
            jnp.where(first_section, slots[4], zero),
            back[0],
            jnp.where(first_section, back[1], slots[4]),
        ]
    )
    both = jnp.concatenate([near, far], axis=2)
    return both.reshape(-1, both.shape[2])


def reduce_errors(features, decoders, dec_bias, targets, live_rows):
    x, y, _, core = coords()
    layers_all, width = dec_bias.shape
    half = live_rows.shape[0] // 2
    rows = half // 4

    def decode(first):
        rebuilt = lax.dot_general(
            decoders, cut(features, 0, first, half), (((1,), (1,)), ((), ())),
            preferred_element_type=F32,
        )
        return rebuilt.reshape(layers_all, width, half)

    arrived = other_core(decode((1 - core) * half))
    kept = decode(core * half)

    def quarter(to):
        return cut(kept, 2, to * rows, rows) + cut(arrived, 2, to * rows, rows)

    parts = [along_y(quarter((y + step) & 3).astype(BF16), step) for step in (1, 3, 2)]
    total = quarter(y)
    for part in parts:
        total = total + part.astype(F32)
    parts = [along_x(pick(total, (x + step) & 3), step) for step in (1, 3, 2)]
    total = pick(total, x)
    for part in parts:
        total = total + part
    first = core * half + y * rows
    wanted = lax.dynamic_slice(targets, (x, first, U32(0)), (1, rows, width))[0].T.astype(F32)
    live = cut(live_rows, 0, first, rows).astype(F32)
    errors = ((total + pick(dec_bias, x)[:, None] - wanted) * live[None, :]).astype(BF16)[None]

    def gather(block, me, axis, shift):
        arrived = [(step, shift(block, step)) for step in (1, 3, 2)]
        size = block.shape[axis]
        shape = list(block.shape)
        shape[axis] *= 4
        whole = put(jnp.zeros(shape, BF16), block, axis, me * size)
        for step, value in arrived:
            whole = put(whole, value, axis, ((me - step) & 3) * size)
        return whole

    errors = gather(errors, x, 0, along_x)
    errors = gather(errors, y, 2, along_y)
    swapped = other_core(errors)
    whole = put(jnp.zeros((layers_all, width, 2 * half), BF16), errors, 2, core * half)
    return put(whole, swapped, 2, (1 - core) * half)


def gradient_kernel(
    where_ref, errors_ref, near_ref, far_ref, early0_ref, early1_ref, late_ref, out_ref
):
    tile = pl.program_id(0)
    section = where_ref[16]
    width, tokens_all = errors_ref.shape[1:]
    scale = 1.0 / tokens_all
    halves = [
        jnp.where(where_ref[8 + 2 * tile + half] == 1, late_ref[...], early_ref[...])
        for half, early_ref in enumerate((early0_ref, early1_ref))
    ]
    near = near_ref[...]
    lead = jnp.where(section == 0, near, jnp.concatenate(halves, axis=1))

    def product(first, count, source):
        residual = errors_ref[pl.ds(first, count)].reshape(count * width, tokens_all)
        value = jnp.dot(residual, source, preferred_element_type=F32) * scale
        return value.astype(BF16).reshape(count, width, source.shape[1])

    out_ref[0:2] = product(2 * section, 2, lead)
    out_ref[2:4] = product(2, 2, near)
    out_ref[4:5] = product(1 + 2 * section, 1, far_ref[...])


def all_gradients(errors, features, early, late):
    _, width, tokens_all = errors.shape
    columns = features.shape[1] // 2
    lanes = late.shape[1]
    z = lax.axis_index("width")
    section = lax.axis_index("section")
    spots = [EARLY.index(behind) if behind in EARLY else 0 for behind in range(8)]
    behind = (z - jnp.arange(8, dtype=jnp.int32)) & 7
    spot = sum(jnp.where(behind == b, spots[b], 0) for b in range(8))
    where = jnp.concatenate([spot, (behind == 4).astype(jnp.int32), section[None].astype(jnp.int32)])
    tiles = columns // (2 * lanes)
    return pl.pallas_call(
        gradient_kernel,
        grid_spec=pltpu.PrefetchScalarGridSpec(
            num_scalar_prefetch=1,
            grid=(tiles,),
            in_specs=[
                pl.BlockSpec(errors.shape, lambda i, where: (0, 0, 0)),
                pl.BlockSpec((tokens_all, 2 * lanes), lambda i, where: (0, i)),
                pl.BlockSpec((tokens_all, 2 * lanes), lambda i, where: (0, tiles + i)),
                pl.BlockSpec((tokens_all, lanes), lambda i, where: (where[2 * i], 0)),
                pl.BlockSpec((tokens_all, lanes), lambda i, where: (where[2 * i + 1], 0)),
                pl.BlockSpec((tokens_all, lanes), lambda i, where: (0, 0)),
            ],
            out_specs=pl.BlockSpec((5, width, 2 * lanes), lambda i, where: (0, 0, i)),
        ),
        out_shape=jax.ShapeDtypeStruct((5, width, columns), BF16),
        cost_estimate=pl.CostEstimate(
            flops=10 * width * tokens_all * columns, bytes_accessed=12000000, transcendentals=0
        ),
        name="gradients",
    )(where, errors, features, features, early, early, late)


def local(mlp_inputs, encoder, enc_bias, decoder, dec_bias, targets, live_rows):
    x, _, _, _ = coords()
    first_section = x < 2
    block = encode(mlp_inputs, encoder, enc_bias)
    decoders = plan_decoders(decoder, first_section)
    blocks = ring_blocks(block)
    early, late = send_ahead(blocks)
    features = assemble(blocks)
    errors = reduce_errors(features, decoders, dec_bias, targets, live_rows)
    gradients = all_gradients(errors, features, early, late)
    return jnp.swapaxes(errors, 1, 2), jnp.swapaxes(gradients, 1, 2)


def solution(mesh):
    placed = (
        P("section", "width", None),
        P("section", "width", "feat"),
        P("section", "feat"),
        P("section", "feat", "width"),
        P(None, "width"),
        P(None, None, "width"),
        P(),
    )
    return jax.shard_map(
        local,
        mesh=mesh,
        in_specs=placed,
        out_specs=(P(None, None, "width"), P("section", "feat", "width")),
        check_vma=False,
    )
```
